256 devices in a mesh: grp: 4 (over x, y), tp: 32 (over z), tower: 2 (over core).
Axes of the slice: x: 2, y: 2, z: 32, core: 2. Of those that a mesh axis runs over, the one named last changes fastest.
The devices are a block of a 4x8x32 slice.
Arguments:
- hidden: bfloat16 [2, 4096, 3072], P('tower', ('grp', 'tp')), parts along dimension 1, may hold values from -6 to 6
- modulation: float32 [2, 3, 3072], P('tower'), may hold values from -3 to 7, as said below
- qk_gains: float32 [2, 3, 4096], P('tower', None, 'tp'), may hold values from 0.75 to 13
- counts: int32 [2, 4], P(None, 'grp'), parts along dimension 1, may hold values from 256 to 1024
- offsets: int32 [2, 4], P(None, 'grp'), parts along dimension 1, may hold values from 0 to 8191
- in_weights: bfloat16 [2, 3072, 4, 4096], P('tower', None, None, 'tp'), may hold values from -0.109375 to 0.109375
- out_weights: bfloat16 [2, 2, 4096, 3072], P('tower', None, 'tp'), may hold values from -0.5 to 0.5
Outputs:
- updated: bfloat16 [2, 4096, 3072], P('tower', ('grp', 'tp')), parts along dimension 1
The draws below stay inside these ranges and needn't reach their ends.
There are 4 independent parts, one for each index of `grp`. The reference program is written for one: setup_inputs(seed, part) draws one part's arguments, and reference() takes and returns one part's arrays. A program takes and returns all parts, laid end to end along the dimension named above; an argument that names none is the same for every part. Nothing has to cross between parts.
Inputs may be any that keep to these rules, and one draw needn't show every extreme that they name: `modulation`: rows are shift, scale and gate.
All inputs are finite; a program needn't handle non-finite values.
Results may differ from the reference program's by a relative error of at most 0.025.
The reference program's roundings to bfloat16 on the way (of `normed`, `projected`, `self_out` and `cross_out`) count: a program that leaves them out, or rounds other values in their place, can miss the bound.
Values may be sent and summed in bfloat16 or wider, within the bound.
No kernel may reach another device: no remote copies, remote signals or barrier semaphores. Data moves between devices by JAX's collectives and lax.ppermute only.
A program may use at most 64 MiB of HBM per device.

```python
import math
import jax
import jax.numpy as jnp
from jax import lax

D = 3072
HD = 128
TOK = 1024
HEADS = 32
HW = 4096
N_TP = 32


def draw_modulation(key, part):
    first_key, second_key, third_key = jax.random.split(key, 3)
    shift = jnp.clip(0.5 * jax.random.normal(first_key, (2, D), jnp.float32), -3.0, 3.0)
    scale = jnp.clip(0.3 * jax.random.normal(second_key, (2, D), jnp.float32), -0.9, 3.0)
    gate = jax.random.uniform(third_key, (2, D), jnp.float32, 0.5, 1.5)
    return jnp.stack([shift, scale, gate], 1).astype(jnp.float32)


def draw_qk_gains(key, part):
    order_key, placing_key, rough_key = jax.random.split(jax.random.fold_in(key, 17), 3)
    ranking = jax.random.permutation(order_key, HEADS).astype(jnp.float32)
    placing = (ranking + jax.random.uniform(placing_key, (HEADS,), jnp.float32)) / HEADS
    top_log = math.log(2.0)
    head_scale = jnp.exp(top_log * placing)
    roughness = jnp.exp(jax.random.uniform(rough_key, (2, 3, HEADS, HD), jnp.float32, -0.25, 0.25))
    return (head_scale[None, None, :, None] * roughness).reshape(2, 3, HW).astype(jnp.float32)


def level_of(own_key, extent, cuts, low, high):
    loudness, own = 1.0, jax.random.fold_in(own_key, 6)
    for dim, parts in cuts:
        draws = jnp.exp(jax.random.uniform(jax.random.fold_in(own, dim), (parts,), jnp.float32, low / len(cuts), high / len(cuts)))
        loudness = loudness * jnp.repeat(draws, extent[dim] // parts).reshape([-1 if axis == dim else 1 for axis in range(len(extent))])
    return loudness


def scatter_about(stream_key, dims, scale, most, shards=(), kind=jnp.bfloat16):
    entries = jax.random.normal(stream_key, dims, jnp.float32) * scale
    if len(shards) > 0:
        entries = level_of(stream_key, dims, shards, -0.22, 0.18) * entries
    return jnp.clip(entries, min=-most, max=most).astype(kind)


def setup_inputs(seed: int = 0, part: int = 0) -> dict:
    splits = jax.random.split(jax.random.key(seed), 8)
    own_keys = jax.random.split(jax.random.fold_in(splits[7], part), 8)
    hidden = scatter_about(own_keys[0], (2, TOK, D), 1.0, 6.0, ((0, 2), (1, 32)))
    modulation = draw_modulation(jax.random.fold_in(splits[7], 71), part)
    qk_gains = draw_qk_gains(jax.random.fold_in(splits[7], 71), part)
    counts = jax.random.randint(own_keys[3], (2, 1), TOK // 4, TOK + 1).astype(jnp.int32)
    offsets = jax.random.randint(own_keys[4], (2, 1), 0, 8192).astype(jnp.int32)
    in_weights = scatter_about(splits[5], (2, D, 4, HW), D ** -0.5, 0.109375, ((0, 2), (3, 32)))
    out_weights = scatter_about(splits[6], (2, 2, HW, D), HD ** -0.5, 0.5, ((0, 2), (2, 32)))
    return {"hidden": hidden, "modulation": modulation, "qk_gains": qk_gains, "counts": counts, "offsets": offsets, "in_weights": in_weights, "out_weights": out_weights}


epsilon = 1e-06
rope_base = 10000.0
masked_score = -1e+30

def layer_norm(states):
    centre = states - lax.optimization_barrier(jnp.mean(states, -1, keepdims=True))
    spread = lax.optimization_barrier(jnp.mean(centre * centre, -1, keepdims=True))
    return centre * lax.rsqrt(spread + epsilon)

def rotate(columns, positions):
    head_width = columns.shape[-1]
    pair_index = jnp.arange(head_width // 2, dtype=jnp.int32)
    frequency = jnp.exp(pair_index.astype(jnp.float32) * (-2.0 * math.log(rope_base) / head_width))
    angles = positions.reshape((positions.shape[0],) + (1,) * (columns.ndim - 1)) * frequency
    cosine = jnp.cos(angles)
    sine_table = jnp.sin(angles)
    even_part = columns[..., 0::2]
    odd_part = columns[..., 1::2]
    turned = jnp.stack([even_part * cosine - odd_part * sine_table, even_part * sine_table + odd_part * cosine], -1)
    return turned.reshape(columns.shape)

def finish(projected, head_gains, positions):
    query_like = jnp.stack([projected[:, 0], projected[:, 1], projected[:, 3]], 1)
    squares = lax.optimization_barrier(jnp.mean(query_like * query_like, -1, keepdims=True))
    query_like = query_like * lax.rsqrt(squares + epsilon) * head_gains[None]
    turned = rotate(query_like, positions)
    return jnp.stack([turned[:, 0], turned[:, 1], projected[:, 2], turned[:, 2]], 1)

def attend(queries, key_rows, value_rows, key_count):
    scores = jnp.dot(queries, key_rows.T, preferred_element_type=jnp.float32) * (1.0 / math.sqrt(queries.shape[-1]))
    usable = jnp.arange(key_rows.shape[0], dtype=jnp.int32) < key_count
    scores = jnp.where(usable[None, :], scores, masked_score)
    row_max = lax.optimization_barrier(jnp.max(scores, -1, keepdims=True))
    raised = jnp.exp(scores - row_max)
    attention = (raised / lax.optimization_barrier(jnp.sum(raised, -1, keepdims=True))).astype(jnp.bfloat16)
    return jnp.dot(attention, value_rows, preferred_element_type=jnp.float32).astype(jnp.bfloat16)

def prepare(tower_index, hidden, modulation, qk_gains, offsets, in_weights):
    states = hidden[tower_index].astype(jnp.float32)
    modulate = modulation[tower_index]
    normed = (layer_norm(states) * (1.0 + modulate[1]) + modulate[0]).astype(jnp.bfloat16)
    projected = jnp.dot(normed, in_weights[tower_index].reshape(D, 4 * HW), preferred_element_type=jnp.float32)
    positions = (offsets[tower_index, 0] + jnp.arange(TOK, dtype=jnp.int32)).astype(jnp.float32)
    head_gains = qk_gains[tower_index].reshape(3, HEADS, HD)
    finished = finish(projected.reshape(TOK, 4, HEADS, HD), head_gains, positions)
    return (states, modulate, finished.astype(jnp.bfloat16))

def heads_attend(queries, key_rows, value_rows, key_count):
    stacked = (jnp.swapaxes(queries, 0, 1), jnp.swapaxes(key_rows, 0, 1), jnp.swapaxes(value_rows, 0, 1))
    result = lax.map(lambda triple: attend(triple[0], triple[1], triple[2], key_count), stacked)
    return jnp.swapaxes(result, 0, 1).reshape(queries.shape[0], HW)

def branch_sum(self_out, cross_out, weights):
    block_width = HW // N_TP

    def accumulate(total_sum, block_index):
        row_start = block_index * block_width
        self_part = lax.dynamic_slice_in_dim(self_out, row_start, block_width, 1)
        cross_part = lax.dynamic_slice_in_dim(cross_out, row_start, block_width, 1)
        self_weight = lax.dynamic_slice_in_dim(weights[0], row_start, block_width, 0)
        cross_weight = lax.dynamic_slice_in_dim(weights[1], row_start, block_width, 0)
        partial_term = jnp.dot(self_part, self_weight, preferred_element_type=jnp.float32) + jnp.dot(cross_part, cross_weight, preferred_element_type=jnp.float32)
        rounded = lax.optimization_barrier(partial_term.astype(jnp.bfloat16))
        return (total_sum + rounded.astype(jnp.float32), None)
    total_sum, unused = lax.scan(accumulate, jnp.zeros((TOK, D), jnp.float32), jnp.arange(N_TP, dtype=jnp.int32))
    return total_sum

def reference(hidden, modulation, qk_gains, counts, offsets, in_weights, out_weights):
    prepared = [prepare(tower_index, hidden, modulation, qk_gains, offsets, in_weights) for tower_index in range(2)]
    outputs = []
    for tower_index in range(2):
        states, modulate, projected = prepared[tower_index]
        opposite = prepared[1 - tower_index][2]
        self_out = heads_attend(projected[:, 0], projected[:, 1], projected[:, 2], counts[tower_index, 0])
        cross_out = heads_attend(projected[:, 3], opposite[:, 1], opposite[:, 2], counts[1 - tower_index, 0])
        branch = branch_sum(self_out, cross_out, out_weights[tower_index])
        outputs.append((states + modulate[2] * branch).astype(jnp.bfloat16))
    return jnp.stack(outputs, 0)
```

```python
import functools
import math

import jax
import jax.numpy as jnp
from jax import lax
from jax.experimental import pallas as pl
from jax.experimental.pallas import tpu as pltpu
from jax.sharding import PartitionSpec as P


epsilon = 1e-06
rope_base = 10000.0
masked_score = -1e30

PIECES = 3


VMEM = pl.BlockSpec(memory_space=pltpu.VMEM)
f32 = jnp.float32
bf16 = jnp.bfloat16


def norm_kernel(hidden_ref, modulation_ref, out_ref):
    states = hidden_ref[...].astype(f32)
    centre = states - jnp.mean(states, -1, keepdims=True)
    spread = jnp.mean(centre * centre, -1, keepdims=True)
    scaled = centre * lax.rsqrt(spread + epsilon)
    out_ref[...] = (scaled * (1.0 + modulation_ref[1:2]) + modulation_ref[0:1]).astype(bf16)


def finish_head(columns, gains, cosine, sine):
    squares = jnp.mean(columns * columns, -1, keepdims=True)
    columns = columns * lax.rsqrt(squares + epsilon) * gains
    width = columns.shape[-1]
    lane = lax.broadcasted_iota(jnp.int32, columns.shape, 1)
    after = pltpu.roll(columns, width - 1, 1)
    before = pltpu.roll(columns, 1, 1)
    swapped = jnp.where(lane % 2 == 0, after, before)
    return (columns * cosine + swapped * sine).astype(bf16)


def project_kernel(starts, with_own, rows, table_at, *refs):
    refs = list(refs)
    pieces = [[refs.pop(0) for _ in range(PIECES)] for _ in starts]
    own_ref = refs.pop(0) if with_own else None
    weight_ref, gains_ref, cos_ref, sin_ref, q_ref, kv_ref = refs
    width = q_ref.shape[1] // 2
    depth = weight_ref.shape[0] // PIECES
    total = None
    for j in range(PIECES):
        parts = [own_ref[:, j * depth : (j + 1) * depth]] if with_own else []
        parts += [step[j][at : at + rows] for step, at in zip(pieces, starts)]
        block = jnp.concatenate(parts, 0)
        term = jnp.dot(block, weight_ref[j * depth : (j + 1) * depth], preferred_element_type=f32)
        total = term if total is None else total + term
    span = slice(table_at, table_at + total.shape[0])
    cosine, sine = cos_ref[span], sin_ref[span]
    q_ref[:, 0:width] = finish_head(total[:, 0:width], gains_ref[0:1], cosine, sine)
    kv_ref[:, 0:width] = finish_head(total[:, width : 2 * width], gains_ref[1:2], cosine, sine)
    kv_ref[:, width : 2 * width] = total[:, 2 * width : 3 * width].astype(bf16)
    q_ref[:, width : 2 * width] = finish_head(total[:, 3 * width :], gains_ref[2:3], cosine, sine)


def attend(queries, key_rows, value_rows, usable):
    scores = lax.dot_general(
        queries, key_rows, (((1,), (1,)), ((), ())), preferred_element_type=f32
    ) * (1.0 / math.sqrt(queries.shape[-1]))
    scores = jnp.where(usable > 0.0, scores, masked_score)
    raised = jnp.exp(scores - jnp.max(scores, -1, keepdims=True))
    weights = raised * (1.0 / jnp.sum(raised, -1, keepdims=True))
    return jnp.dot(weights.astype(bf16), value_rows, preferred_element_type=f32).astype(bf16)


def attend_kernel(n_kv, layouts, other_span, rows, spans, *refs):
    refs = list(refs)
    own_q, other_q = refs.pop(0), refs.pop(0)
    local = [refs.pop(0) for _ in range(n_kv)]
    foreign = [refs.pop(0) for _ in range(n_kv)]
    usable_ref = refs.pop(0)
    weight_refs = (refs.pop(0), refs.pop(0))
    keys, values, asked, answered = refs[-4:]
    outs = refs[:-4]
    width = keys.shape[2]
    k_columns, v_columns = slice(0, width), slice(width, 2 * width)
    at = [0, 0]
    for parts, flip in ((local, 0), (foreign, 1)):
        for part, layout in zip(parts, layouts):
            start = 0
            for tower, size in layout:
                to = tower ^ flip
                keys[to, at[to] : at[to] + size] = part[start : start + size, k_columns]
                values[to, at[to] : at[to] + size] = part[start : start + size, v_columns]
                at[to] += size
                start += size
    edge = own_q.shape[0]
    count = asked.shape[1]
    asked[0, 0:edge] = own_q[:, k_columns]
    asked[1, 0:edge] = own_q[:, v_columns]
    asked[0, edge:count] = other_q[other_span[0] : other_span[1], v_columns]
    asked[1, edge:count] = other_q[other_span[0] : other_span[1], k_columns]
    tile = next(t for t in (128, 96, 80, 64, 32) if count % t == 0)
    tiles = count // tile

    @pl.loop(0, 2 * tiles)
    def _(step):
        tower = step // tiles
        at = pl.multiple_of((step % tiles) * tile, 16)
        answered[tower, pl.ds(at, tile)] = attend(
            asked[tower, pl.ds(at, tile)],
            keys[tower],
            values[tower],
            usable_ref[pl.ds(tower, 1)],
        )

    own_both = jnp.concatenate([answered[0, 0:edge], answered[1, 0:edge]], 1)
    other_both = jnp.concatenate([answered[1, edge:count], answered[0, edge:count]], 1)
    own_term = jnp.dot(own_both, weight_refs[0][...], preferred_element_type=f32).astype(bf16)
    other_term = jnp.dot(other_both, weight_refs[1][...], preferred_element_type=f32).astype(bf16)
    outs = list(outs)
    for own_at, other_at in spans:
        for j in range(PIECES):
            out = outs.pop(0)
            columns = slice(j * out.shape[1], (j + 1) * out.shape[1])
            at = 0
            if own_at is not None:
                out[0:rows] = own_term[own_at : own_at + rows, columns]
                at = rows
            if other_at is not None:
                out[at : at + rows] = other_term[other_at : other_at + rows, columns]


def wrap(blocks, n):
    blocks = jnp.where(blocks >= n, blocks - n, blocks)
    return jnp.where(blocks < 0, blocks + n, blocks)


def tables_kernel(n, rows, counts_ref, offsets_ref, cos_own, sin_own, cos_other, sin_other, usable_ref):
    place, side = lax.axis_index("tp"), lax.axis_index("tower")
    sign = 2 * side - 1
    size, width = cos_own.shape
    row = lax.broadcasted_iota(jnp.int32, (size, width), 0)
    lane = lax.broadcasted_iota(jnp.int32, (size, width), 1)
    frequency = jnp.exp((lane // 2).astype(f32) * (-2.0 * math.log(rope_base) / width))
    for offset, nearest, cos_ref, sin_ref in (
        (offsets_ref[side, 0], 1, cos_own, sin_own),
        (offsets_ref[1 - side, 0], 0, cos_other, sin_other),
    ):
        block = wrap(place + sign * (nearest + row // rows), n)
        angles = (offset + block * rows + row % rows).astype(f32) * frequency
        cos_ref[...] = jnp.cos(angles)
        sine = jnp.sin(angles)
        sin_ref[...] = jnp.where(lane % 2 == 0, -sine, sine)
    keys = usable_ref.shape[1]
    key = lax.broadcasted_iota(jnp.int32, (1, keys), 1)
    foreign = key >= size
    within = jnp.where(foreign, key - size, key)
    direction = jnp.where(foreign, -sign, sign)
    for tower, count in ((0, counts_ref[side, 0]), (1, counts_ref[1 - side, 0])):
        nearest = jnp.where(foreign, tower, 1 - tower)
        block = wrap(place + direction * (nearest + within // rows), n)
        real = block * rows + within % rows < count
        usable_ref[tower : tower + 1] = jnp.where(real, 1.0, 0.0)


def call(kernel, outs, flops, limit, args, scratch=(), specs=None):
    return pl.pallas_call(
        kernel,
        out_shape=outs,
        in_specs=specs or [VMEM] * len(args),
        out_specs=[VMEM] * len(outs),
        scratch_shapes=list(scratch),
        cost_estimate=pl.CostEstimate(flops=flops, bytes_accessed=1 << 20, transcendentals=0),
        compiler_params=pltpu.CompilerParams(vmem_limit_bytes=limit << 20),
    )(*args)


def block(hidden, modulation, qk_gains, counts, offsets, in_weights, out_weights):
    n = lax.axis_size("tp")
    rows, model_width = hidden.shape[1:]
    head_width = in_weights.shape[-1]
    towers = lax.axis_size("tower")
    shape = jax.ShapeDtypeStruct

    def flat(s, t):
        return (s % n) * towers + t

    outward = [(flat(s, t), flat(s + 1 - 2 * t, t)) for s in range(n) for t in range(2)]
    inward = [(b, a) for a, b in outward]
    across = [(0, 1), (1, 0)]

    def ring(value, pairs):
        return lax.ppermute(value, ("tp", "tower"), pairs)

    def swap(value):
        return lax.ppermute(value, "tower", across)

    (normed,) = call(
        norm_kernel,
        [shape((rows, model_width), bf16)],
        10 * rows * model_width,
        8,
        (hidden[0], modulation[0]),
    )
    other_normed = swap(normed)
    piece_width = model_width // PIECES
    message = jnp.concatenate([normed, other_normed], 0)
    pieces = [message[:, j * piece_width : (j + 1) * piece_width] for j in range(PIECES)]

    far = n // 2
    size = far * rows
    tables = call(
        functools.partial(tables_kernel, n, rows),
        [shape((size, head_width), f32)] * 4 + [shape((2, 2 * size), f32)],
        100 * size * head_width,
        8,
        (counts, offsets),
        specs=[pl.BlockSpec(memory_space=pltpu.SMEM)] * 2,
    )
    usable = tables[4]

    steps = {}
    for d in range(1, far + 1):
        if d == far:
            pieces = [p[0:rows] for p in pieces]
        pieces = [ring(p, outward) for p in pieces]
        if d == 1:
            pieces, in_weights, out_weights = lax.optimization_barrier((pieces, in_weights, out_weights))
        steps[d] = pieces

    weights = [in_weights[0].reshape(model_width, 4 * head_width)]
    weights.append(swap(weights[0]))
    out_weights = [out_weights[0].reshape(2 * head_width, model_width)]
    out_weights.append(swap(out_weights[0]))
    gains = [qk_gains[0]]
    gains.append(swap(gains[0]))

    own_dists, other_dists = batches_of(far)
    q, kv = [[], []], [[], []]
    for tower, batches in enumerate((own_dists, other_dists)):
        for b, dists in enumerate(batches):
            count = rows * len(dists)
            away = [d for d in dists if d > 0]
            args = [p for d in away for p in steps[d]]
            if 0 in dists:
                args.append(other_normed)
            args += [weights[tower], gains[tower], *tables[2 * tower : 2 * tower + 2]]
            result = call(
                functools.partial(
                    project_kernel,
                    (tower * rows,) * len(away),
                    0 in dists,
                    rows,
                    rows * (dists[0] - (1 - tower)),
                ),
                [shape((count, 2 * head_width), bf16)] * 2,
                2 * count * model_width * 4 * head_width,
                16,
                args,
            )
            q[tower].append(result[0])
            kv[tower].append(result[1])

    n_own, n_other = len(own_dists), len(other_dists)
    cuts = [0, n_own // 3 + 1, n_own - 2, n_own]
    local_kv, foreign_kv, layouts = [], [], []
    for g in range(3):
        parts, layout = [], []
        for tower, last in ((0, n_own), (1, n_other)):
            for b in range(cuts[g], min(cuts[g + 1], last)):
                parts.append(kv[tower][b])
                layout.append((tower, kv[tower][b].shape[0]))
        local_kv.append(jnp.concatenate(parts, 0))
        foreign_kv.append(swap(local_kv[-1]))
        layouts.append(tuple(layout))

    terms = {}
    for g in range(n_own):
        b = n_own - 1 - g
        own = own_dists[b]
        source = min(b, n_other - 1)
        held = other_dists[source]
        other = [d for d in held if d in own or d == 0]
        dists = sorted(set(own) | set(other))
        spans, outs = [], []
        for d in dists:
            spans.append(
                (
                    rows * own.index(d) if d in own else None,
                    rows * other.index(d) if d in other else None,
                )
            )
            height = rows * ((d in own) + (d in other))
            outs += [shape((height, piece_width), bf16)] * PIECES
        count = rows * (len(own) + len(other))
        first = rows * held.index(other[0])
        args = [q[0][b], q[1][source]] + local_kv + foreign_kv + [usable, *out_weights]
        result = call(
            functools.partial(
                attend_kernel,
                len(layouts),
                tuple(layouts),
                (first, first + rows * len(other)),
                rows,
                tuple(spans),
            ),
            outs,
            4 * count * (2 * n * rows * head_width + head_width * model_width),
            16,
            args,
            scratch=[pltpu.VMEM((2, 2 * size, head_width), bf16)] * 2
            + [pltpu.VMEM((2, count, head_width), bf16)] * 2,
        )
        for i, d in enumerate(dists):
            terms[d] = result[PIECES * i : PIECES * (i + 1)]

    def add(part, term):
        return (part.astype(f32) + term.astype(f32)).astype(bf16)

    sums = [ring(p, inward) for p in terms[far]]
    for d in reversed(range(1, far)):
        added = []
        for part, term in zip(sums, terms[d]):
            if part.shape[0] == rows:
                added.append(jnp.concatenate([add(part, term[0:rows]), term[rows:]], 0))
            else:
                added.append(add(part, term))
        sums = [ring(p, inward) for p in added]
    other_sum = [add(p[rows:], t) for p, t in zip(sums, terms[0])]
    arrived = swap(jnp.concatenate(other_sum, 1))
    own_sum = jnp.concatenate([p[0:rows] for p in sums], 1)
    branch = own_sum.astype(f32) + arrived.astype(f32)
    return (hidden[0].astype(f32) + modulation[0, 2] * branch).astype(bf16)[None]


def batches_of(far):
    own = [[d, d + 1] for d in range(1, far, 2)]
    other = [list(pair) for pair in own[:-1]]
    other[0] = [0] + other[0]
    other[-1].append(far - 1)
    return own, other


def solution(mesh):
    return jax.shard_map(
        block,
        mesh=mesh,
        in_specs=(
            P("tower", ("grp", "tp"), None),
            P("tower", None, None),
            P("tower", None, "tp"),
            P(None, "grp"),
            P(None, "grp"),
            P("tower", None, None, "tp"),
            P("tower", None, "tp", None),
        ),
        out_specs=P("tower", ("grp", "tp"), None),
        check_vma=False,
    )
```
